512 devices in a mesh: gx: 16 (over z_lo, core), gy: 4 (over x), gz: 8 (over y, z_hi).
Axes of the slice: x: 4, y: 4, z: 16 (z_hi: 2, z_lo: 8; z = z_hi * 8 + z_lo), core: 2. Of those that a mesh axis runs over, the one named last changes fastest.
Arguments:
- features: float32 [16, 4, 8, 256, 256], P('gx', 'gy', 'gz'), may hold values from -6 to 6
- positions: float32 [16, 4, 8, 3, 256], P('gx', 'gy', 'gz'), may hold values from 0 to 1
- counts: int32 [16, 4, 8], P('gx', 'gy', 'gz'), may hold values from 51 to 256, as said below
- w_src: float32 [256, 256], replicated, may hold values from -0.375 to 0.375
- w_out: float32 [256, 256], replicated, may hold values from -0.375 to 0.375
- radial: float32 [8, 256], replicated, may hold values from -5 to 5
Outputs:
- updated: float32 [16, 4, 8, 256, 256], P('gx', 'gy', 'gz')
The draws below stay inside these ranges and needn't reach their ends.
Inputs may be any that keep to these rules, and one draw needn't show every extreme that they name: The atoms of a bin fill its first counts slots; some bin is full in every draw, and some bins hold more than 128 atoms.
All inputs are finite; a program needn't handle non-finite values.
Results may differ from the reference program's by a relative error of at most 0.0003.
Values sent between devices are 32-bit elements; how exact they have to be, the bound alone decides.
No kernel may reach another device: no remote copies, remote signals or barrier semaphores. Data moves between devices by JAX's collectives and lax.ppermute only.
A program may use at most 64 MiB of HBM per device.

```python
import jax
import jax.numpy as jnp
from jax import lax

F = 256
NRBF = 8
CAP = 256
BLK = 128
BINS_X = 16
BINS_Y = 4
BINS_Z = 8


def draw_counts(key, part):
    key_light, key_dense, key_pick, key_spot = jax.random.split(jax.random.fold_in(key, 17), 4)
    grid_shape = (BINS_X, BINS_Y, BINS_Z)
    light_counts = jax.random.randint(key_light, grid_shape, CAP // 5, BLK + 1)
    dense_counts = jax.random.randint(key_dense, grid_shape, BLK + 1, CAP + 1)
    is_dense = jax.random.randint(key_pick, grid_shape, 0, 8) == 0
    values_flat = jnp.where(is_dense, dense_counts, light_counts).reshape(-1)
    full_bin = jax.random.randint(key_spot, (), 0, BINS_X * BINS_Y * BINS_Z)
    values_flat = jnp.where(jnp.arange(BINS_X * BINS_Y * BINS_Z) == full_bin, CAP, values_flat)
    return values_flat.reshape(grid_shape).astype(jnp.int32)


def steps_of(own_key, extent, pieces, smallest, top_value):
    def one(axis_at, blocks):
        steps = jax.random.uniform(jax.random.fold_in(jax.random.fold_in(own_key, 6), axis_at), (blocks,), jnp.float32, smallest / len(pieces), top_value / len(pieces))
        return jnp.repeat(jnp.exp(steps), extent[axis_at] // blocks).reshape((-1,) + (1,) * (len(extent) - axis_at - 1))

    level = one(*pieces[0])
    for cut in pieces[1:]:
        level = level * one(*cut)
    return level


def noise(rng, extent, scale, reach, cuts=(), held_as=jnp.bfloat16):
    loudness = steps_of(rng, extent, cuts, -0.22, 0.18) if cuts else 1.0
    result = jax.random.normal(rng, extent, jnp.float32) * scale * loudness
    return jnp.minimum(jnp.maximum(result, -reach), reach).astype(held_as)


def setup_inputs(seed: int = 0) -> dict:
    arg_keys = jax.random.split(jax.random.key(seed), 7)
    features = noise(arg_keys[0], (BINS_X, BINS_Y, BINS_Z, CAP, F), 1.0, 6.0, ((0, 16), (1, 4), (2, 8)), jnp.float32)
    positions = jnp.clip(1.0 * jax.random.uniform(arg_keys[1], (BINS_X, BINS_Y, BINS_Z, 3, CAP), jnp.float32) ** steps_of(arg_keys[1], (BINS_X, BINS_Y, BINS_Z, 3, CAP), ((0, 16), (1, 4), (2, 8)), -0.2, 0.2), 0.0, 1.0)
    counts = draw_counts(jax.random.fold_in(arg_keys[6], 71), 0)
    w_src = noise(arg_keys[3], (F, F), F ** -0.5, 0.375, (), jnp.float32)
    w_out = noise(arg_keys[4], (F, F), F ** -0.5, 0.375, (), jnp.float32)
    radial = noise(arg_keys[5], (NRBF, F), 1.0, 5.0, (), jnp.float32)
    return {"features": features, "positions": positions, "counts": counts, "w_src": w_src, "w_out": w_out, "radial": radial}


far_value = 100.0
gamma_width = 10.0
message_scale = 0.125
highest = lax.Precision.HIGHEST

def offset_of(task_index):
    return jnp.stack([task_index // 9, task_index // 3 % 3, task_index % 3]).astype(jnp.float32) - 1.0

def radial_terms(left_pos, right_pos, right_feats, offset, same_bin, row_block, col_block, radial):
    rows_left = lax.dynamic_slice_in_dim(left_pos, row_block * BLK, BLK, 1)
    rows_right = lax.dynamic_slice_in_dim(right_pos, col_block * BLK, BLK, 1) + offset[:, None]
    separation = rows_right[:, None, :] - rows_left[:, :, None]
    distance = jnp.sqrt(lax.optimization_barrier(jnp.sum(separation * separation, axis=0)))
    envelope = jnp.where(distance < 1.0, 0.5 * (jnp.cos(jnp.pi * distance) + 1.0), 0.0)
    diagonal = lax.broadcasted_iota(jnp.int32, (BLK, BLK), 0) == lax.broadcasted_iota(jnp.int32, (BLK, BLK), 1)
    envelope = jnp.where(diagonal & same_bin & (row_block == col_block), 0.0, envelope)
    centres = (lax.broadcasted_iota(jnp.float32, (1, NRBF, 1), 1) + 0.5) / NRBF
    radial_basis = envelope[:, None, :] * jnp.exp(-gamma_width * (distance[:, None, :] - centres) ** 2)
    feature_rows = lax.dynamic_slice_in_dim(right_feats, col_block * BLK, BLK, 0)
    weighted = (radial[:, None, :] * feature_rows[None, :, :]).reshape(NRBF * BLK, feature_rows.shape[1])
    return jnp.dot(radial_basis.reshape(BLK, NRBF * BLK), weighted, precision=highest, preferred_element_type=jnp.float32)

def task_sum(left_pos, right_pos, right_feats, offset, same_bin, left_blocks, right_blocks, radial, running):
    divisor = jnp.maximum(right_blocks, 1)

    def add_pair(counter, partial_sum):
        row_block = counter // divisor
        col_block = counter % divisor
        term = radial_terms(left_pos, right_pos, right_feats, offset, same_bin, row_block, col_block, radial)
        current = lax.dynamic_slice_in_dim(partial_sum, row_block * BLK, BLK, 0)
        return lax.dynamic_update_slice_in_dim(partial_sum, current + term, row_block * BLK, 0)
    return lax.fori_loop(0, left_blocks * right_blocks, add_pair, running)

def reference(features, positions, counts, w_src, w_out, radial):
    bin_total = BINS_X * BINS_Y * BINS_Z
    width = features.shape[-1]
    flat_feats = features.reshape(bin_total * CAP, width)
    projected = jnp.dot(flat_feats, w_src, precision=highest, preferred_element_type=jnp.float32)
    projected = projected.reshape(BINS_X, BINS_Y, BINS_Z, CAP, width)
    slot_index = jnp.arange(CAP, dtype=jnp.int32)
    placed = jnp.where(slot_index[None, None, None, None, :] < counts[:, :, :, None, None], positions, far_value)
    blocks = (counts + BLK - 1) // BLK

    def bin_message(bin_index):
        coord_x = bin_index // (BINS_Y * BINS_Z)
        coord_y = bin_index // BINS_Z % BINS_Y
        coord_z = bin_index % BINS_Z

        def add_task(task_index, running):
            near_x = (coord_x + task_index // 9 - 1) % BINS_X
            near_y = (coord_y + task_index // 3 % 3 - 1) % BINS_Y
            near_z = (coord_z + task_index % 3 - 1) % BINS_Z
            return task_sum(placed[coord_x, coord_y, coord_z], placed[near_x, near_y, near_z], projected[near_x, near_y, near_z], offset_of(task_index), task_index == 13, blocks[coord_x, coord_y, coord_z], blocks[near_x, near_y, near_z], radial, running)
        return lax.fori_loop(0, 27, add_task, jnp.zeros((CAP, width), jnp.float32))
    message = lax.map(bin_message, jnp.arange(bin_total, dtype=jnp.int32))
    mixed = jnp.dot(message_scale * message.reshape(bin_total * CAP, width), w_out, precision=highest, preferred_element_type=jnp.float32)
    return (flat_feats + jax.nn.silu(mixed)).reshape(features.shape)
```

```python
import functools
import math

import jax
import jax.numpy as jnp
from jax import lax
from jax.experimental import pallas as pl
from jax.experimental.pallas import tpu as pltpu
from jax.sharding import PartitionSpec as P

F = 256
NRBF = 8
CAP = 256
BLK = 128
ROWS = CAP + 8
CHUNK = 16

far_value = 100.0
gamma_width = 10.0
message_scale = 0.125
highest = lax.Precision.HIGHEST
f32 = jnp.float32
bf16 = jnp.bfloat16

centres = [(k + 0.5) / NRBF for k in range(NRBF)]
centre_factor = [math.exp(-gamma_width * c * c) for c in centres]
log2e = 1.0 / math.log(2.0)
step_rate = 2.0 * gamma_width / NRBF * log2e
base_rate = 2.0 * gamma_width * centres[0] * log2e
square_rate = gamma_width * log2e
envelope_q = (
    -4.311447075915581e-05,
    0.0008613919314042151,
    -0.011120371504262472,
    0.0945534332328893,
    -0.46740107023744926,
    0.999999999671398,
)


def split(value):
    high = value.astype(bf16)
    return high, (value - high.astype(f32)).astype(bf16)


def round_up(value, unit):
    return (value + unit - 1) // unit * unit


def pack_kernel(count_ref, feats_ref, pos_ref, w_ref, out_ref):
    count = count_ref[0]
    out_ref[0:CAP, :] = jnp.dot(
        feats_ref[...], w_ref[...], precision=highest, preferred_element_type=f32
    )
    slot = lax.broadcasted_iota(jnp.int32, (1, CAP), 1)
    for axis in range(3):
        out_ref[CAP + axis : CAP + axis + 1, :] = jnp.where(
            slot < count, pos_ref[axis : axis + 1, :], far_value
        )
    out_ref[CAP + 3 : CAP + 4, :] = jnp.full((1, CAP), count.astype(f32))
    out_ref[CAP + 4 : CAP + 8, :] = jnp.zeros((4, CAP), f32)


def basis_rows(xi, yi, zi, xj, yj, zj):
    dx = xj - xi
    dy = yj - yi
    dz = zj - zi
    square = jnp.clip(dx * dx + dy * dy + dz * dz, 1e-30, 1.0)
    distance = square * lax.rsqrt(square)
    rest = 1.0 - square
    envelope = envelope_q[0]
    for coefficient in envelope_q[1:]:
        envelope = envelope * square + coefficient
    envelope = (rest * rest) * envelope
    factor = jnp.exp2(step_rate * distance)
    value = envelope * jnp.exp2(base_rate * distance - square_rate * square)
    yield value
    for _ in range(NRBF - 1):
        value = value * factor
        yield value


def message_kernel(shifts, moves, adds, oz_ref, radial_ref, *refs):
    targets = len(shifts)
    sources = len(moves)
    refs = list(refs)
    target_refs = [refs.pop(0) for _ in range(targets)]
    source_refs = [refs.pop(0) for _ in range(sources)]
    prior_refs = [refs.pop(0) for _ in range(targets)] if adds else [None] * targets
    out_refs = [refs.pop(0) for _ in range(targets)]
    tx, ty, tz, feats, spots, w_high, w_low, left, total = refs
    oz = oz_ref[0]
    row8 = lax.broadcasted_iota(jnp.int32, (8, CAP), 0)

    begins = []
    counts = []
    begin = jnp.int32(0)
    for shift, ref in zip(shifts, target_refs):
        packet = ref[ref.shape[0] - 8 :, :]
        count = jnp.max(packet[3:4, 0:BLK]).astype(jnp.int32)
        columns = jnp.transpose(packet)
        where = pl.ds(pl.multiple_of(begin, 8), CAP)
        tx[where, :] = jnp.broadcast_to(columns[:, 0:1] + float(shift), (CAP, BLK))
        ty[where, :] = jnp.broadcast_to(columns[:, 1:2], (CAP, BLK))
        tz[where, :] = jnp.broadcast_to(columns[:, 2:3], (CAP, BLK))
        begins.append(begin)
        counts.append(count)
        begin = begin + round_up(count, 8)
    row_blocks = (begin + BLK - 1) // BLK

    begin = jnp.int32(0)
    for (move_y, sign_z), ref in zip(moves, source_refs):
        packet = ref[CAP : CAP + 8, :]
        count = jnp.max(packet[3:4, 0:BLK]).astype(jnp.int32)
        offset = jnp.where(row8 == 1, float(move_y), jnp.where(row8 == 2, sign_z * oz, 0.0))
        where = pl.ds(pl.multiple_of(begin, 8), CAP)
        feats[where, :] = ref[0:CAP, :]
        spots[where, 0:8] = jnp.transpose(packet + offset)
        begin = begin + round_up(count, 8)
        last = begin
    tail = pl.ds(pl.multiple_of(last, 8), BLK)
    feats[tail, :] = jnp.zeros((BLK, F), f32)
    spots[tail, :] = jnp.full((BLK, BLK), far_value, f32)
    column_blocks = (begin + BLK - 1) // BLK

    total[...] = jnp.zeros_like(total)

    @pl.loop(0, column_blocks)
    def _(column_block):
        here = pl.ds(pl.multiple_of(column_block * BLK, BLK), BLK)
        block = feats[here, :]
        for k in range(NRBF):
            weighted = block * (radial_ref[k : k + 1, :] * centre_factor[k])
            high, low = split(weighted)
            w_high[k * BLK : (k + 1) * BLK, :] = high
            w_low[k * BLK : (k + 1) * BLK, :] = low
        across = jnp.transpose(spots[here, :])
        xj = jnp.broadcast_to(across[0:1, :], (CHUNK, BLK))
        yj = jnp.broadcast_to(across[1:2, :], (CHUNK, BLK))
        zj = jnp.broadcast_to(across[2:3, :], (CHUNK, BLK))

        @pl.loop(0, row_blocks)
        def _(row_block):
            first = pl.multiple_of(row_block * BLK, BLK)
            for chunk in range(BLK // CHUNK):
                rows = pl.ds(first + chunk * CHUNK, CHUNK)
                values = basis_rows(tx[rows, :], ty[rows, :], tz[rows, :], xj, yj, zj)
                for k, value in enumerate(values):
                    high, low = split(value)
                    into = slice(chunk * CHUNK, (chunk + 1) * CHUNK)
                    left[into, k * BLK : (k + 1) * BLK] = high
                    left[into, (NRBF + k) * BLK : (NRBF + k + 1) * BLK] = low
            rows = pl.ds(first, BLK)
            upper = left[:, : NRBF * BLK]
            lower = left[:, NRBF * BLK :]
            term = jnp.dot(upper, w_high[...], preferred_element_type=f32)
            term += jnp.dot(upper, w_low[...], preferred_element_type=f32)
            term += jnp.dot(lower, w_high[...], preferred_element_type=f32)
            total[rows, :] += term

    slot = lax.broadcasted_iota(jnp.int32, (CAP, 1), 0)
    for out_ref, prior_ref, begin, count in zip(out_refs, prior_refs, begins, counts):
        part = total[pl.ds(pl.multiple_of(begin, 8), CAP), :]
        part = jnp.where(slot < count, part, 0.0)
        out_ref[...] = part if prior_ref is None else part + prior_ref[...]


def messages(shifts, moves, oz, radial, target_packets, source_packets, priors=()):
    targets, sources = len(shifts), len(moves)
    target_rows = targets * CAP + BLK
    source_rows = sources * CAP + BLK
    vmem = pl.BlockSpec(memory_space=pltpu.VMEM)
    arrays = [radial, *target_packets, *source_packets, *priors]
    pairs = targets * sources
    return pl.pallas_call(
        functools.partial(message_kernel, shifts, moves, bool(priors)),
        out_shape=[jax.ShapeDtypeStruct((CAP, F), f32)] * targets,
        in_specs=[pl.BlockSpec(memory_space=pltpu.SMEM)] + [vmem] * len(arrays),
        out_specs=[vmem] * targets,
        scratch_shapes=[
            pltpu.VMEM((target_rows, BLK), f32),
            pltpu.VMEM((target_rows, BLK), f32),
            pltpu.VMEM((target_rows, BLK), f32),
            pltpu.VMEM((source_rows, F), f32),
            pltpu.VMEM((source_rows, BLK), f32),
            pltpu.VMEM((NRBF * BLK, F), bf16),
            pltpu.VMEM((NRBF * BLK, F), bf16),
            pltpu.VMEM((BLK, 2 * NRBF * BLK), bf16),
            pltpu.VMEM((target_rows, F), f32),
        ],
        cost_estimate=pl.CostEstimate(
            flops=pairs * 6 * BLK * NRBF * BLK * F,
            bytes_accessed=4 * F * CAP * (targets + sources),
            transcendentals=3 * pairs * BLK * BLK,
        ),
        compiler_params=pltpu.CompilerParams(vmem_limit_bytes=24 * 1024 * 1024),
    )(oz, *arrays)


def final_kernel(feats_ref, packet_ref, own_ref, left_ref, right_ref, radial_ref, w_ref, out_ref):
    count = jnp.max(packet_ref[CAP + 3 : CAP + 4, 0:BLK]).astype(jnp.int32)
    live = (count + BLK - 1) // BLK * BLK
    slot = lax.broadcasted_iota(jnp.int32, (CAP, 1), 0)
    projected = packet_ref[0:CAP, :]
    rho = jnp.zeros((1, F), f32)
    for k in range(NRBF):
        rho = rho + radial_ref[k : k + 1, :] * centre_factor[k]
    empty = (slot >= count) & (slot < live)
    empty_sum = jnp.sum(jnp.where(empty, projected, 0.0), axis=0, keepdims=True)
    itself = jnp.where(empty, empty_sum, 0.0) - jnp.where(slot < live, projected, 0.0)
    message = own_ref[...] + left_ref[...] + right_ref[...] + rho * itself
    mixed = jnp.dot(
        message_scale * message, w_ref[...], precision=highest, preferred_element_type=f32
    )
    out_ref[...] = feats_ref[...] + mixed / (1.0 + jnp.exp(-mixed))


def local(sizes, features, positions, counts, w_src, w_out, radial):
    count_x, count_y, count_z = sizes
    vmem = pl.BlockSpec(memory_space=pltpu.VMEM)
    smem = pl.BlockSpec(memory_space=pltpu.SMEM)
    feats = features[0, 0, 0]
    own = pl.pallas_call(
        pack_kernel,
        out_shape=jax.ShapeDtypeStruct((ROWS, F), f32),
        in_specs=[smem, vmem, vmem, vmem],
        out_specs=vmem,
        cost_estimate=pl.CostEstimate(
            flops=12 * CAP * F * F, bytes_accessed=3 * 4 * CAP * F, transcendentals=0
        ),
    )(counts.reshape(1), feats, positions[0, 0, 0], w_src)

    ring = lambda n, by: [(i, (i + by) % n) for i in range(n)]
    even = lax.axis_index("gz") % 2 == 0
    oz = jnp.where(even, 1.0, -1.0).astype(f32).reshape(1)

    swapped = lax.ppermute(own, "gz", [(i, i ^ 1) for i in range(count_z)])
    below = lax.ppermute(own, "gy", ring(count_y, 1))
    above = lax.ppermute(own, "gy", ring(count_y, -1))
    spots = own[CAP:]
    spots_before = lax.ppermute(spots, "gx", ring(count_x, 1))
    spots_after = lax.ppermute(spots, "gx", ring(count_x, -1))
    target_packets = [spots_before, own, spots_after]

    first = messages(
        (-1, 0, 1),
        ((0, 0), (-1, 0), (1, 0)),
        oz,
        radial,
        target_packets,
        [own, below, above],
    )

    def hop(move_y, move_z):
        pairs = []
        for y in range(count_y):
            for z in range(count_z):
                over = (z + (2 if z % 2 == 0 else -2) * move_z) % count_z
                pairs.append((y * count_z + z, (y + move_y) % count_y * count_z + over))
        return lax.ppermute(swapped, ("gy", "gz"), pairs)

    near = [hop(1, 0), hop(-1, 0), hop(0, 1), hop(1, 1), hop(-1, 1)]
    near_moves = ((-1, 1), (1, 1), (0, -1), (-1, -1), (1, -1))

    second = messages((-1, 0, 1), ((0, 1),), oz, radial, target_packets, [swapped], first)
    before, after = messages(
        (-1, 1), near_moves, oz, radial, [spots_before, spots_after], near, [second[0], second[2]]
    )
    from_after = lax.ppermute(before, "gx", ring(count_x, -1))
    from_before = lax.ppermute(after, "gx", ring(count_x, 1))
    (here,) = messages((0,), near_moves, oz, radial, [own], near, [second[1]])

    out = pl.pallas_call(
        final_kernel,
        out_shape=jax.ShapeDtypeStruct((CAP, F), f32),
        in_specs=[vmem] * 7,
        out_specs=vmem,
        cost_estimate=pl.CostEstimate(
            flops=12 * CAP * F * F, bytes_accessed=7 * 4 * CAP * F, transcendentals=CAP * F
        ),
    )(feats, own, here, from_after, from_before, radial, w_out)
    return out[None, None, None]


def solution(mesh):
    in_specs = (
        P("gx", "gy", "gz", None, None),
        P("gx", "gy", "gz", None, None),
        P("gx", "gy", "gz"),
        P(),
        P(),
        P(),
    )
    out_specs = P("gx", "gy", "gz", None, None)
    sizes = tuple(mesh.shape[axis] for axis in ("gx", "gy", "gz"))
    return jax.shard_map(
        functools.partial(local, sizes), mesh=mesh, in_specs=in_specs, out_specs=out_specs, check_vma=False
    )
```
